32 devices in a mesh: gx: 8 (over z, core), gy: 4 (over y, x).
Axes of the slice: x: 2, y: 2, z: 4, core: 2. Of those that a mesh axis runs over, the one named last changes fastest.
Arguments:
- velocity: float32 [3, 128, 64, 128], P(None, 'gx', 'gy'), may hold values from -6 to 6
- stresses: float32 [6, 128, 64, 128], P(None, 'gx', 'gy'), may hold values from -6 to 6
- buoyancy: float32 [128, 64, 128], P('gx', 'gy'), may hold values from 0.3 to 0.6
- lame_first: float32 [128, 64, 128], P('gx', 'gy'), may hold values from 0.05 to 0.15
- rigidity: float32 [128, 64, 128], P('gx', 'gy'), may hold values from 0.04 to 0.12
- histories: bfloat16 [8192, 512], P(('gx', 'gy')), may hold values from -6 to 6
- mechanism: bfloat16 [8192, 6], P(('gx', 'gy')), may hold values from -6 to 6
- resample: bfloat16 [512, 3], replicated, may hold values from -0.25 to 0.25
- owners: int32 [8192, 1], P(('gx', 'gy')), may hold values from 0 to 3; in each aligned block of 256 rows (0 to 255, 256 to 511, ...) at most 64 rows name the same one
- cell_offsets: int32 [8192], P(('gx', 'gy')), may hold values from 0 to 32767
Outputs:
- velocity_out: float32 [3, 128, 64, 128], P(None, 'gx', 'gy')
- stresses_out: float32 [6, 128, 64, 128], P(None, 'gx', 'gy')
The draws below stay inside these ranges and needn't reach their ends.
Inputs may be any that keep to these rules, and one draw needn't show every extreme that they name: `owners`: among the 256 rows of one device at most 64 name the same owner, a bound that some block reaches of them. `cell_offsets`: cell index x * 16 * 128 + y * 128 + z within the enclosing block.
All inputs are finite; a program needn't handle non-finite values.
Results may differ from the reference program's by a relative error of at most 0.00052.
Values may be sent and summed in bfloat16 or wider, within the bound.
A program may use at most 64 MiB of HBM per device.

```python
import math
import jax
import jax.numpy as jnp
import numpy as np
from jax import lax

CX = 16
CY = 16
CZ = 128
STEPS = 3
SAMPLES = 512
SRC_DEV = 256
CAP = 64
NX = 128
NY = 64
SOURCES = 8192
N_GY = 4


def plant(values, stream_key, least, high):
    shape = values.shape
    place = [jax.random.randint(jax.random.fold_in(stream_key, axis), (), 0, shape[axis]) for axis in range(len(shape))]
    values = values.at[tuple(place)].set(least)
    longest = shape.index(max(shape))
    place[longest] = (place[longest] + 1) % shape[longest]
    return values.at[tuple(place)].set(high)


def block_levels(rng, dims, shards, least, high):
    def one(position, blocks):
        heights = jax.random.uniform(jax.random.fold_in(jax.random.fold_in(rng, 6), position), (blocks,), jnp.float32, least / len(shards), high / len(shards))
        return jnp.repeat(jnp.exp(heights), dims[position] // blocks).reshape((-1,) + (1,) * (len(dims) - position - 1))

    gain = one(*shards[0])
    for cut in shards[1:]:
        gain = gain * one(*cut)
    return gain


def routed_block(key, own, number, rows, count, top, bound, skew):
    sequence = jax.random.permutation(key, count)
    packed, ordinary = shares(count, rows * top, bound, skew, True), shares(count, rows * top, bound, skew, False)
    places = jnp.arange(count)

    def named(lengths, turn):
        used = int((lengths > 0).sum())
        fixed = max(1, used // 4)
        moved = fixed + (places - fixed + turn * (used - fixed)) % max(1, count - fixed)
        return jnp.zeros((count,), jnp.int32).at[sequence[jnp.where(places < fixed, places, moved)]].set(jnp.asarray(lengths, jnp.int32))

    lengths = jnp.where(number % 4 == 0, named(packed, number // 4), named(ordinary, number - number // 4 - 1))
    mixed = jax.random.permutation(jax.random.fold_in(own, 3), count)
    donor, taker = mixed[0:count // 2 * 2:2], mixed[1:count // 2 * 2:2]
    margin = jnp.minimum(lengths[donor] - 1, bound - lengths[taker]) // 2
    margin = jnp.where((donor == sequence[0]) | (taker == sequence[0]) | (lengths[taker] == 0), 0, jnp.maximum(margin, 0))
    moved = jax.random.randint(jax.random.fold_in(own, 4), (count // 2,), 0, 1 << 20) % (margin + 1)
    lengths = lengths.at[donor].add(-moved).at[taker].add(moved)
    items = jnp.searchsorted(jnp.cumsum(lengths), jnp.arange(rows * top), side="right").astype(jnp.int32)
    table = items.reshape(top, rows).T
    table = table[jax.random.permutation(jax.random.fold_in(own, 1), rows)]
    turn = jax.random.randint(jax.random.fold_in(own, 2), (rows, 1), 0, top)
    return jnp.take_along_axis(table, (jnp.arange(top)[None, :] + turn) % top, axis=1)


def shares(number_of, total, bound, skew, full):
    portions = [(1 << 20) // math.isqrt(standing ** skew) + 1 for standing in range(1, number_of + 1)]
    largest = bound if full else min(bound, max(-(-total // number_of), total * portions[0] // sum(portions)))
    least = 1 if total - largest >= number_of - 1 else 0
    counts, spare = [largest] + [least] * (number_of - 1), total - largest - least * (number_of - 1)
    while spare > 0:
        movable = [i for i in range(1, number_of) if counts[i] < largest] or [i for i in range(1, number_of) if counts[i] < bound]
        whole, left = sum([portions[i] for i in movable]), spare
        for i in movable:
            extra = min(bound - counts[i], max(1, left * portions[i] // whole), spare)
            counts[i] = counts[i] + extra
            spare = spare - extra
    return np.array(counts)


def noise(stream_key, dims, width, limit, split=(), kind=jnp.bfloat16):
    drawn = jax.random.normal(stream_key, dims, jnp.float32) * width
    if len(split) > 0:
        drawn = block_levels(stream_key, dims, split, -0.22, 0.18) * drawn
    return jnp.clip(drawn, min=-limit, max=limit).astype(kind)


def setup_inputs(seed: int = 0) -> dict:
    arg_keys = jax.random.split(jax.random.key(seed), 11)
    velocity = noise(arg_keys[0], (3, NX, NY, CZ), 1.0, 6.0, ((1, 8), (2, 4)), jnp.float32)
    stresses = noise(arg_keys[1], (6, NX, NY, CZ), 1.0, 6.0, ((1, 8), (2, 4)), jnp.float32)
    buoyancy = jnp.clip(jnp.exp(math.log(0.6) - 0.6931472 * jax.random.uniform(arg_keys[2], (NX, NY, CZ), jnp.float32) ** block_levels(arg_keys[2], (NX, NY, CZ), ((0, 8), (1, 4)), -0.2, 0.2)), 0.3, 0.6)
    lame_first = jnp.clip(0.05 + 0.10000001 * jax.random.uniform(arg_keys[3], (NX, NY, CZ), jnp.float32) ** block_levels(arg_keys[3], (NX, NY, CZ), ((0, 8), (1, 4)), -0.2, 0.2), 0.05, 0.15)
    rigidity = jnp.clip(jnp.exp(math.log(0.12) - 1.0986123 * jax.random.uniform(arg_keys[4], (NX, NY, CZ), jnp.float32) ** block_levels(arg_keys[4], (NX, NY, CZ), ((0, 8), (1, 4)), -0.2, 0.2)), 0.04, 0.12)
    histories = noise(arg_keys[5], (SOURCES, SAMPLES), 1.0, 6.0, ((0, 32),))
    mechanism = noise(arg_keys[6], (SOURCES, 6), 1.0, 6.0, ((0, 32),))
    resample = noise(arg_keys[7], (SAMPLES, STEPS), SAMPLES ** -0.5, 0.25)
    owners_keys = jax.random.split(jax.random.fold_in(arg_keys[8], 1), SOURCES // SRC_DEV)
    owners_turns = jax.random.permutation(jax.random.fold_in(arg_keys[8], 3), SOURCES // SRC_DEV)
    owners = jax.vmap(lambda own, number: routed_block(jax.random.fold_in(arg_keys[8], 2), own, number, SRC_DEV, N_GY, 1, CAP, 2))(owners_keys, owners_turns).reshape((SOURCES, 1))
    cell_offsets = plant(jax.random.randint(arg_keys[9], (SOURCES,), 0, CX * CY * CZ), jax.random.fold_in(arg_keys[9], 1), 0, (CX * CY * CZ) - 1).astype(jnp.int32)
    return {"velocity": velocity, "stresses": stresses, "buoyancy": buoyancy, "lame_first": lame_first, "rigidity": rigidity, "histories": histories, "mechanism": mechanism, "resample": resample, "owners": owners, "cell_offsets": cell_offsets}


INNER_WEIGHT = 9.0 / 8.0
OUTER_WEIGHT = -1.0 / 24.0


def differ(values, dimension, forward):
    if dimension == 2:
        values = jnp.pad(values, ((0, 0), (0, 0), (2, 2)))
    extent = values.shape[dimension] - 4

    def window(start_at):
        return lax.slice_in_dim(values, start_at, start_at + extent, axis=dimension)

    if forward:
        result = INNER_WEIGHT * (window(3) - window(2)) + OUTER_WEIGHT * (window(4) - window(1))
    else:
        result = INNER_WEIGHT * (window(2) - window(1)) + OUTER_WEIGHT * (window(3) - window(0))
    for second in (0, 1):
        if second != dimension:
            result = lax.slice_in_dim(result, 2, result.shape[second] - 2, axis=second)
    return result


def advance_velocity(velocity, stresses, buoyancy):
    forces = jnp.stack([
        differ(stresses[0], 0, True) + differ(stresses[3], 1, False) + differ(stresses[4], 2, False),
        differ(stresses[3], 0, False) + differ(stresses[1], 1, True) + differ(stresses[5], 2, False),
        differ(stresses[4], 0, False) + differ(stresses[5], 1, False) + differ(stresses[2], 2, True),
    ])
    return velocity + buoyancy * forces


def advance_stress(stresses, velocity, lame_first, rigidity):
    stretch_one = differ(velocity[0], 0, False)
    stretch_two = differ(velocity[1], 1, False)
    stretch_three = differ(velocity[2], 2, False)
    change = stretch_one + stretch_two + stretch_three
    rates = jnp.stack([
        lame_first * change + 2.0 * rigidity * stretch_one,
        lame_first * change + 2.0 * rigidity * stretch_two,
        lame_first * change + 2.0 * rigidity * stretch_three,
        rigidity * (differ(velocity[0], 1, True) + differ(velocity[1], 0, True)),
        rigidity * (differ(velocity[0], 2, True) + differ(velocity[2], 0, True)),
        rigidity * (differ(velocity[1], 2, True) + differ(velocity[2], 1, True)),
    ])
    return stresses + rates


def reference(velocity, stresses, buoyancy, lame_first, rigidity, histories, mechanism, resample, owners, cell_offsets):
    amplitude = jnp.dot(histories, resample, preferred_element_type=jnp.float32)
    terms = (mechanism.astype(jnp.float32)[:, :, None] * amplitude[:, None, :]).astype(jnp.bfloat16)
    device = jnp.arange(SOURCES, dtype=jnp.int32) // SRC_DEV
    across_cells = (device // N_GY) * CX + cell_offsets // (CY * CZ)
    normal_cells = owners[:, 0] * CY + (cell_offsets // CZ) % CY
    depth_cells = cell_offsets % CZ
    border = ((0, 0), (2, 2), (2, 2), (0, 0))
    for step_index in range(STEPS):
        velocity = advance_velocity(velocity, jnp.pad(stresses, border), buoyancy)
        stresses = advance_stress(stresses, jnp.pad(velocity, border), lame_first, rigidity)
        stresses = stresses.at[:, across_cells, normal_cells, depth_cells].add(terms[:, :, step_index].astype(jnp.float32).T)
    return velocity, stresses
```

```python
import functools

import jax
import jax.numpy as jnp
from jax import lax
from jax.experimental import pallas as pl
from jax.experimental.pallas import tpu as pltpu
from jax.sharding import PartitionSpec as P

A = 9.0 / 8.0
B = -1.0 / 24.0
MESH = pl.DeviceIdType.MESH
XP = 2
YP = 8

STRESS_FACES = (((0, True), (3, False), (4, False)), ((3, False), (1, True), (5, False)))
VELOCITY_FACES = (((0, False), (1, True), (2, True)), ((0, True), (1, False), (2, True)))


def face_layers(faces, up, extent):
    out = []
    for comp, forward in faces:
        if up:
            out += [(comp, extent - 1)] + ([] if forward else [(comp, extent - 2)])
        else:
            out += [(comp, 0)] + ([(comp, 1)] if forward else [])
    return out


def halo_terms(faces, from_low, extent, halo):
    out, at = [], 0
    for comp, forward in faces:
        first = halo(at)
        if from_low:
            if forward:
                out.append((comp, 0, -B * first))
                at += 1
            else:
                second = halo(at + 1)
                out.append((comp, 0, -A * first - B * second))
                out.append((comp, 1, -B * first))
                at += 2
        else:
            if forward:
                second = halo(at + 1)
                out.append((comp, extent - 1, A * first + B * second))
                out.append((comp, extent - 2, B * first))
                at += 2
            else:
                out.append((comp, extent - 1, B * first))
                at += 1
    return out


def kernel(
    groups, blocks, steps,
    v_hbm, s_hbm, buoy_hbm, lame_hbm, rig_hbm, hist_hbm, mech_ref, res_ref, own_ref, off_ref,
    vo_hbm, so_hbm,
    V, S, buoy, lame, rig, hist, src, gathered, plane_hot, level_hot,
    send_x, recv_x, send_y, recv_y,
    load_sem, store_sem, src_send, src_recv, face_send, face_recv,
):
    gx = lax.axis_index("gx")
    gy = lax.axis_index("gy")
    cx, cy, cz = buoy.shape
    rows = hist.shape[0]
    inner = (slice(None), pl.ds(XP, cx), pl.ds(YP, cy), slice(None))

    barrier = pltpu.get_barrier_semaphore()
    sides = (
        (gx > 0, (gx - 1, gy)),
        (gx < blocks - 1, (gx + 1, gy)),
        (gy > 0, (gx, gy - 1)),
        (gy < groups - 1, (gx, gy + 1)),
    )
    for there, device in sides[:2]:
        @pl.when(there)
        def _(device=device):
            pl.semaphore_signal(barrier, inc=1, device_id=device, device_id_type=MESH)
    for k in range(1, groups):
        pl.semaphore_signal(
            barrier, inc=1, device_id=(gx, lax.rem(gy + k, groups)), device_id_type=MESH
        )

    loads = [
        pltpu.make_async_copy(s_hbm, S.at[inner], load_sem.at[0]),
        pltpu.make_async_copy(hist_hbm, hist, load_sem.at[1]),
        pltpu.make_async_copy(v_hbm, V.at[inner], load_sem.at[2]),
        pltpu.make_async_copy(buoy_hbm, buoy, load_sem.at[3]),
        pltpu.make_async_copy(lame_hbm, lame, load_sem.at[4]),
        pltpu.make_async_copy(rig_hbm, rig, load_sem.at[5]),
    ]
    for load in loads:
        load.start()

    for ref in (V, S):
        zero_x = jnp.zeros((ref.shape[0], XP, cy, cz), jnp.float32)
        ref[:, pl.ds(0, XP), pl.ds(YP, cy), :] = zero_x
        ref[:, pl.ds(XP + cx, XP), pl.ds(YP, cy), :] = zero_x

        def clear(x, carry, ref=ref):
            zero_y = jnp.zeros((ref.shape[0], YP, cz), jnp.float32)
            ref[:, XP + x, pl.ds(0, YP), :] = zero_y
            ref[:, XP + x, pl.ds(YP + cy, YP), :] = zero_y
            return carry

        lax.fori_loop(0, cx, clear, 0)

    def face_copy(phase, side, faces):
        axis, up = side // 2, side % 2
        send, recv = ((send_x, recv_x), (send_y, recv_y))[axis]
        count = len(face_layers(faces[axis], bool(up), (cx, cy)[axis]))
        return pltpu.make_async_remote_copy(
            src_ref=send.at[phase, up, pl.ds(0, count)],
            dst_ref=recv.at[phase, up, pl.ds(0, count)],
            send_sem=face_send.at[phase, side],
            recv_sem=face_recv.at[phase, side],
            device_id=sides[side][1],
            device_id_type=MESH,
        )

    def row(ref, comp, axis, layer):
        if axis == 0:
            return ref.at[comp, XP + layer, pl.ds(YP, cy), :]
        return ref.at[comp, pl.ds(XP, cx), YP + layer, :]

    def coefficient(ref, axis, layer):
        return ref[layer] if axis == 0 else ref[:, layer, :]

    def send_faces(phase, ref, faces):
        for side in (3, 2, 1, 0):
            axis, up = side // 2, side % 2
            send = (send_x, send_y)[axis]

            @pl.when(sides[side][0])
            def _():
                for at, (comp, layer) in enumerate(
                    face_layers(faces[axis], bool(up), (cx, cy)[axis])
                ):
                    send[phase, up, at] = row(ref, comp, axis, layer)[...]
                face_copy(phase, side, faces).start()

    def receive_faces(phase, faces, apply):
        for side in (0, 1, 2, 3):
            axis, up = side // 2, side % 2
            recv = (recv_x, recv_y)[axis]

            @pl.when(sides[side][0])
            def _():
                face_copy(phase, 2 * axis + 1 - up, faces).wait_recv()
                for comp, layer, value in halo_terms(
                    faces[axis], not up, (cx, cy)[axis], lambda at: recv[phase, 1 - up, at]
                ):
                    apply(axis, comp, layer, value)

    def finish_faces(phase, faces):
        for side in (0, 1, 2, 3):
            @pl.when(sides[side][0])
            def _():
                face_copy(phase, side, faces).wait_send()

    def add(ref, comp, axis, layer, value):
        place = row(ref, comp, axis, layer)
        place[...] = place[...] + value

    force_of = ({0: 0, 3: 1, 4: 2}, {3: 0, 1: 1, 5: 2})

    def apply_force(axis, comp, layer, value):
        add(V, force_of[axis][comp], axis, layer, coefficient(buoy, axis, layer) * value)

    shear_of = ({1: 3, 2: 4}, {0: 3, 2: 5})

    def apply_strain(axis, comp, layer, value):
        mu = coefficient(rig, axis, layer)
        if comp != axis:
            add(S, shear_of[axis][comp], axis, layer, mu * value)
            return
        volume = coefficient(lame, axis, layer) * value
        for normal in range(3):
            extra = volume + 2.0 * mu * value if normal == axis else volume
            add(S, normal, axis, layer, extra)

    level = lax.broadcasted_iota(jnp.int32, (cy, cz), 1)

    def along_z(values, by):
        moved = pltpu.roll(values, (-by) % cz, 1)
        return jnp.where(level < cz - by if by > 0 else level >= -by, moved, 0.0)

    def differ(ref, comp, x, dimension, forward):
        def window(by):
            if dimension == 0:
                return ref[comp, XP + x + by, pl.ds(YP, cy), :]
            if dimension == 1:
                return ref[comp, XP + x, pl.ds(YP + by, cy), :]
            values = ref[comp, XP + x, pl.ds(YP, cy), :]
            return along_z(values, by) if by else values

        if forward:
            return A * (window(1) - window(0)) + B * (window(2) - window(-1))
        return A * (window(0) - window(-1)) + B * (window(1) - window(-2))

    def velocity_inner(x, carry):
        force = (
            differ(S, 0, x, 0, True) + differ(S, 3, x, 1, False) + differ(S, 4, x, 2, False),
            differ(S, 3, x, 0, False) + differ(S, 1, x, 1, True) + differ(S, 5, x, 2, False),
            differ(S, 4, x, 0, False) + differ(S, 5, x, 1, False) + differ(S, 2, x, 2, True),
        )
        factor = buoy[x]
        for comp in range(3):
            place = V.at[comp, XP + x, pl.ds(YP, cy), :]
            place[...] = place[...] + factor * force[comp]
        return carry

    def stress_inner(x, carry):
        one = differ(V, 0, x, 0, False)
        two = differ(V, 1, x, 1, False)
        three = differ(V, 2, x, 2, False)
        mu = rig[x]
        volume = lame[x] * (one + two + three)
        rates = (
            volume + 2.0 * mu * one,
            volume + 2.0 * mu * two,
            volume + 2.0 * mu * three,
            mu * (differ(V, 0, x, 1, True) + differ(V, 1, x, 0, True)),
            mu * (differ(V, 0, x, 2, True) + differ(V, 2, x, 0, True)),
            mu * (differ(V, 1, x, 2, True) + differ(V, 2, x, 1, True)),
        )
        for comp in range(6):
            place = S.at[comp, XP + x, pl.ds(YP, cy), :]
            place[...] = place[...] + rates[comp]
        return carry

    def source_copy(k):
        return pltpu.make_async_remote_copy(
            src_ref=src,
            dst_ref=gathered.at[:, pl.ds(k * rows, rows)],
            send_sem=src_send.at[k],
            recv_sem=src_recv.at[k],
            device_id=(gx, lax.rem(gy + k, groups)),
            device_id_type=MESH,
        )

    def source_terms():
        contract_last = (((1,), (1,)), ((), ()))
        amplitude = lax.dot_general(
            res_ref[...], hist[...], contract_last, preferred_element_type=jnp.float32
        )
        comps = mech_ref.shape[0]
        parts = [mech_ref[...].astype(jnp.float32) * amplitude[t : t + 1, :] for t in range(steps)]
        offsets = off_ref[...]
        places = [own_ref[...], offsets // (cy * cz), (offsets // cz) % cy, offsets % cz]
        places = [p.astype(jnp.float32) for p in places]
        parts += [jnp.concatenate(places + [jnp.zeros((comps - 4, rows), jnp.float32)], axis=0)]
        packed = jnp.concatenate(parts, axis=0).astype(jnp.bfloat16)
        src[...] = packed
        gathered[:, pl.ds(0, rows)] = packed

    comps = mech_ref.shape[0]

    def source_masks():
        for k in range(groups):
            lanes = pl.ds(k * rows, rows)
            info = gathered[pl.ds(steps * comps, comps), lanes].astype(jnp.float32)
            cell_plane = info[0:1] * float(cx * cy) + info[1:2] * float(cy) + info[2:3]
            plane = lax.broadcasted_iota(jnp.int32, (cx * cy, rows), 0) + gy * (cx * cy)
            plane_hot[:, lanes] = jnp.where(
                plane == cell_plane.astype(jnp.int32), 1.0, 0.0
            ).astype(jnp.bfloat16)
            height = lax.broadcasted_iota(jnp.int32, (cz, rows), 0)
            level_hot[:, lanes] = jnp.where(
                height == info[3:4].astype(jnp.int32), 1.0, 0.0
            ).astype(jnp.bfloat16)

    def insert_sources(t):
        values = gathered[pl.ds(t * comps, comps), :].astype(jnp.float32)
        for comp in range(0, 6, 2):
            spread = jnp.concatenate(
                [
                    level_hot[...] * values[c : c + 1, :].astype(jnp.bfloat16)
                    for c in (comp, comp + 1)
                ],
                axis=0,
            )
            placed = lax.dot_general(
                plane_hot[...], spread, (((1,), (1,)), ((), ())),
                preferred_element_type=jnp.float32,
            )
            for c in range(2):
                place = S.at[comp + c, pl.ds(XP, cx), pl.ds(YP, cy), :]
                place[...] = place[...] + placed[:, c * cz : (c + 1) * cz].reshape(cx, cy, cz)

    arrivals = (
        (gx > 0).astype(jnp.int32) + (gx < blocks - 1).astype(jnp.int32) + (groups - 1)
    )
    loads[0].wait()
    pl.semaphore_wait(barrier, arrivals)
    for t in range(steps):
        first, second = 2 * t, 2 * t + 1
        send_faces(first, S, STRESS_FACES)
        if t == 0:
            loads[1].wait()
            source_terms()
            for k in range(1, groups):
                source_copy(k).start()
            loads[2].wait()
            loads[3].wait()
        lax.fori_loop(0, cx, velocity_inner, 0)
        if t > 0:
            insert_sources(t)
        receive_faces(first, STRESS_FACES, apply_force)
        send_faces(second, V, VELOCITY_FACES)
        if t == steps - 1:
            store_v = pltpu.make_async_copy(V.at[inner], vo_hbm, store_sem.at[0])
            store_v.start()
        if t == 0:
            loads[4].wait()
            loads[5].wait()
        lax.fori_loop(0, cx, stress_inner, 0)
        if t == 0:
            for k in range(1, groups):
                source_copy(k).wait_recv()
            source_masks()
            insert_sources(0)
        receive_faces(second, VELOCITY_FACES, apply_strain)
    store_s = pltpu.make_async_copy(S.at[inner], so_hbm, store_sem.at[1])
    store_s.start()
    for t in range(steps):
        finish_faces(2 * t, STRESS_FACES)
        finish_faces(2 * t + 1, VELOCITY_FACES)
    for k in range(1, groups):
        source_copy(k).wait_send()
    store_v.wait()
    store_s.wait()


def local(
    velocity, stresses, buoyancy, lame_first, rigidity,
    histories, mechanism, resample, owners, cell_offsets,
):
    groups = lax.axis_size("gy")
    blocks = lax.axis_size("gx")
    rows, samples = histories.shape
    steps = resample.shape[1]
    _, cx, cy, cz = velocity.shape
    comps = 8
    tall = comps * (steps + 1)
    f32, bf16 = jnp.float32, jnp.bfloat16
    mech = jnp.pad(mechanism.T, ((0, comps - mechanism.shape[1]), (0, 0)))
    res = jnp.pad(resample.T, ((0, -steps % 8), (0, 0)))
    hbm = pl.BlockSpec(memory_space=pl.ANY)
    vmem = pl.BlockSpec(memory_space=pltpu.VMEM)
    dma = pltpu.SemaphoreType.DMA
    phases = 2 * steps
    return pl.pallas_call(
        functools.partial(kernel, groups, blocks, steps),
        out_shape=(
            jax.ShapeDtypeStruct(velocity.shape, f32),
            jax.ShapeDtypeStruct(stresses.shape, f32),
        ),
        in_specs=[hbm] * 6 + [vmem] * 4,
        out_specs=(hbm, hbm),
        scratch_shapes=[
            pltpu.VMEM((3, cx + 2 * XP, cy + 2 * YP, cz), f32),
            pltpu.VMEM((6, cx + 2 * XP, cy + 2 * YP, cz), f32),
            pltpu.VMEM((cx, cy, cz), f32),
            pltpu.VMEM((cx, cy, cz), f32),
            pltpu.VMEM((cx, cy, cz), f32),
            pltpu.VMEM((rows, samples), bf16),
            pltpu.VMEM((tall, rows), bf16),
            pltpu.VMEM((tall, groups * rows), bf16),
            pltpu.VMEM((cx * cy, groups * rows), bf16),
            pltpu.VMEM((cz, groups * rows), bf16),
            pltpu.VMEM((phases, 2, 5, cy, cz), f32),
            pltpu.VMEM((phases, 2, 5, cy, cz), f32),
            pltpu.VMEM((phases, 2, 5, cx, cz), f32),
            pltpu.VMEM((phases, 2, 5, cx, cz), f32),
            dma((6,)),
            dma((2,)),
            dma((groups,)),
            dma((groups,)),
            dma((phases, 4)),
            dma((phases, 4)),
        ],
        compiler_params=pltpu.CompilerParams(collective_id=0, has_side_effects=True),
    )(
        velocity, stresses, buoyancy, lame_first, rigidity, histories, mech, res,
        owners.reshape(1, rows), cell_offsets.reshape(1, rows),
    )


def solution(mesh):
    in_specs = (
        P(None, "gx", "gy", None),
        P(None, "gx", "gy", None),
        P("gx", "gy", None),
        P("gx", "gy", None),
        P("gx", "gy", None),
        P(("gx", "gy"), None),
        P(("gx", "gy"), None),
        P(),
        P(("gx", "gy"), None),
        P(("gx", "gy")),
    )
    out_specs = (P(None, "gx", "gy", None), P(None, "gx", "gy", None))
    return jax.shard_map(local, mesh=mesh, in_specs=in_specs, out_specs=out_specs, check_vma=False)
```

```python
import functools

import jax
import jax.numpy as jnp
from jax import lax
from jax.experimental import pallas as pl
from jax.experimental.pallas import tpu as pltpu
from jax.sharding import PartitionSpec as P

A = 9.0 / 8.0
B = -1.0 / 24.0
MESH = pl.DeviceIdType.MESH
XP = 2
YP = 8

STRESS_FACES = (((0, True), (3, False), (4, False)), ((3, False), (1, True), (5, False)))
VELOCITY_FACES = (((0, False), (1, True), (2, True)), ((0, True), (1, False), (2, True)))


def face_layers(faces, up, extent):
    out = []
    for comp, forward in faces:
        if up:
            out += [(comp, extent - 1)] + ([] if forward else [(comp, extent - 2)])
        else:
            out += [(comp, 0)] + ([(comp, 1)] if forward else [])
    return out


def halo_terms(faces, from_low, extent, halo):
    out, at = [], 0
    for comp, forward in faces:
        first = halo(at)
        if from_low:
            if forward:
                out.append((comp, 0, -B * first))
                at += 1
            else:
                second = halo(at + 1)
                out.append((comp, 0, -A * first - B * second))
                out.append((comp, 1, -B * first))
                at += 2
        else:
            if forward:
                second = halo(at + 1)
                out.append((comp, extent - 1, A * first + B * second))
                out.append((comp, extent - 2, B * first))
                at += 2
            else:
                out.append((comp, extent - 1, B * first))
                at += 1
    return out


def kernel(
    groups, blocks, steps,
    v_hbm, s_hbm, buoy_hbm, lame_hbm, rig_hbm, hist_hbm, mech_hbm, res_hbm, own_hbm, off_hbm,
    v_out, s_out,
    V, S, buoy, lame, rig, hist, mech_ref, res_ref, own_ref, off_ref, src, gathered, plane_hot, level_hot,
    send_x, recv_x, send_y, recv_y,
    load_sem, src_send, src_recv, face_send, face_recv,
):
    gx = lax.axis_index("gx")
    gy = lax.axis_index("gy")
    cx, cy, cz = buoy.shape
    rows = hist.shape[0]
    inner = (slice(None), pl.ds(XP, cx), pl.ds(YP, cy), slice(None))

    barrier = pltpu.get_barrier_semaphore()
    sides = (
        (gx > 0, (gx - 1, gy)),
        (gx < blocks - 1, (gx + 1, gy)),
        (gy > 0, (gx, gy - 1)),
        (gy < groups - 1, (gx, gy + 1)),
    )
    for there, device in sides[:2]:
        @pl.when(there)
        def _(device=device):
            pl.semaphore_signal(barrier, inc=1, device_id=device, device_id_type=MESH)
    for k in range(1, groups):
        pl.semaphore_signal(
            barrier, inc=1, device_id=(gx, lax.rem(gy + k, groups)), device_id_type=MESH
        )

    loads = [
        pltpu.make_async_copy(s_hbm, S.at[inner], load_sem.at[0]),
        pltpu.make_async_copy(hist_hbm, hist, load_sem.at[1]),
        pltpu.make_async_copy(v_hbm, V.at[inner], load_sem.at[2]),
        pltpu.make_async_copy(buoy_hbm, buoy, load_sem.at[3]),
        pltpu.make_async_copy(lame_hbm, lame, load_sem.at[4]),
        pltpu.make_async_copy(rig_hbm, rig, load_sem.at[5]),
        pltpu.make_async_copy(mech_hbm, mech_ref, load_sem.at[6]),
        pltpu.make_async_copy(res_hbm, res_ref, load_sem.at[7]),
        pltpu.make_async_copy(own_hbm, own_ref, load_sem.at[8]),
        pltpu.make_async_copy(off_hbm, off_ref, load_sem.at[9]),
    ]
    for load in loads:
        load.start()

    for ref in (V, S):
        zero_x = jnp.zeros((ref.shape[0], XP, cy, cz), jnp.float32)
        ref[:, pl.ds(0, XP), pl.ds(YP, cy), :] = zero_x
        ref[:, pl.ds(XP + cx, XP), pl.ds(YP, cy), :] = zero_x

        def clear(x, carry, ref=ref):
            zero_y = jnp.zeros((ref.shape[0], YP, cz), jnp.float32)
            ref[:, XP + x, pl.ds(0, YP), :] = zero_y
            ref[:, XP + x, pl.ds(YP + cy, YP), :] = zero_y
            return carry

        lax.fori_loop(0, cx, clear, 0)

    def face_copy(phase, side, faces):
        axis, up = side // 2, side % 2
        send, recv = ((send_x, recv_x), (send_y, recv_y))[axis]
        count = len(face_layers(faces[axis], bool(up), (cx, cy)[axis]))
        return pltpu.make_async_remote_copy(
            src_ref=send.at[phase, up, pl.ds(0, count)],
            dst_ref=recv.at[phase, up, pl.ds(0, count)],
            send_sem=face_send.at[phase, side],
            recv_sem=face_recv.at[phase, side],
            device_id=sides[side][1],
            device_id_type=MESH,
        )

    def row(ref, comp, axis, layer):
        x, y = (XP, YP) if ref is V or ref is S else (0, 0)
        if axis == 0:
            return ref.at[comp, x + layer, pl.ds(y, cy), :]
        return ref.at[comp, pl.ds(x, cx), y + layer, :]

    def coefficient(ref, axis, layer):
        return ref[layer] if axis == 0 else ref[:, layer, :]

    odd = lax.rem(gy, 2) == 1
    even = jnp.logical_not(odd)
    near = ((2, jnp.logical_and(sides[2][0], odd)), (3, jnp.logical_and(sides[3][0], even)))
    far = ((3, jnp.logical_and(sides[3][0], odd)), (2, jnp.logical_and(sides[2][0], even)))
    across = ((0, sides[0][0]), (1, sides[1][0]))

    def send_face(side, phase, ref, faces):
        axis, up = side // 2, side % 2
        send = (send_x, send_y)[axis]
        for at, (comp, layer) in enumerate(face_layers(faces[axis], bool(up), (cx, cy)[axis])):
            send[phase, up, at] = row(ref, comp, axis, layer)[...]
        face_copy(phase, side, faces).start()

    def receive_face(side, phase, faces, apply):
        axis, up = side // 2, side % 2
        recv = (recv_x, recv_y)[axis]
        face_copy(phase, 2 * axis + 1 - up, faces).wait_recv()
        for comp, layer, value in halo_terms(
            faces[axis], not up, (cx, cy)[axis], lambda at: recv[phase, 1 - up, at]
        ):
            apply(axis, comp, layer, value)

    def at_sides(which, *actions):
        for side, there in which:
            @pl.when(there)
            def _(side=side):
                for action in actions:
                    action(side)

    def exchange(phase, faces, apply, send):
        def receive(side):
            receive_face(side, phase, faces, apply)

        at_sides(across, receive)
        at_sides(near, receive, *send)
        at_sides(far, receive, *send)
        at_sides(across, *send)

    def finish_faces(phase, faces):
        for side in (0, 1, 2, 3):
            @pl.when(sides[side][0])
            def _(side=side):
                face_copy(phase, side, faces).wait_send()

    def add(ref, comp, axis, layer, value):
        place = row(ref, comp, axis, layer)
        place[...] = place[...] + value

    force_of = ({0: 0, 3: 1, 4: 2}, {3: 0, 1: 1, 5: 2})

    def apply_force(axis, comp, layer, value):
        add(V, force_of[axis][comp], axis, layer, coefficient(buoy, axis, layer) * value)

    shear_of = ({1: 3, 2: 4}, {0: 3, 2: 5})

    def apply_strain(target, axis, comp, layer, value):
        mu = coefficient(rig, axis, layer)
        if comp != axis:
            add(target, shear_of[axis][comp], axis, layer, mu * value)
            return
        volume = coefficient(lame, axis, layer) * value
        for normal in range(3):
            extra = volume + 2.0 * mu * value if normal == axis else volume
            add(target, normal, axis, layer, extra)

    level = lax.broadcasted_iota(jnp.int32, (cy, cz), 1)

    def along_z(values, by):
        moved = pltpu.roll(values, (-by) % cz, 1)
        return jnp.where(level < cz - by if by > 0 else level >= -by, moved, 0.0)

    def differ(ref, comp, x, dimension, forward):
        def window(by):
            if dimension == 0:
                return ref[comp, XP + x + by, pl.ds(YP, cy), :]
            if dimension == 1:
                return ref[comp, XP + x, pl.ds(YP + by, cy), :]
            values = ref[comp, XP + x, pl.ds(YP, cy), :]
            return along_z(values, by) if by else values

        if forward:
            return A * (window(1) - window(0)) + B * (window(2) - window(-1))
        return A * (window(0) - window(-1)) + B * (window(1) - window(-2))

    def velocity_inner(x, carry):
        force = (
            differ(S, 0, x, 0, True) + differ(S, 3, x, 1, False) + differ(S, 4, x, 2, False),
            differ(S, 3, x, 0, False) + differ(S, 1, x, 1, True) + differ(S, 5, x, 2, False),
            differ(S, 4, x, 0, False) + differ(S, 5, x, 1, False) + differ(S, 2, x, 2, True),
        )
        factor = buoy[x]
        for comp in range(3):
            place = V.at[comp, XP + x, pl.ds(YP, cy), :]
            place[...] = place[...] + factor * force[comp]
        return carry

    def stress_inner(last, x, carry):
        one = differ(V, 0, x, 0, False)
        two = differ(V, 1, x, 1, False)
        three = differ(V, 2, x, 2, False)
        mu = rig[x]
        volume = lame[x] * (one + two + three)
        rates = (
            volume + 2.0 * mu * one,
            volume + 2.0 * mu * two,
            volume + 2.0 * mu * three,
            mu * (differ(V, 0, x, 1, True) + differ(V, 1, x, 0, True)),
            mu * (differ(V, 0, x, 2, True) + differ(V, 2, x, 0, True)),
            mu * (differ(V, 1, x, 2, True) + differ(V, 2, x, 1, True)),
        )
        for comp in range(6):
            place = S.at[comp, XP + x, pl.ds(YP, cy), :]
            target = s_out.at[comp, x] if last else place
            target[...] = place[...] + rates[comp]
        if last:
            for comp in range(3):
                v_out[comp, x] = V[comp, XP + x, pl.ds(YP, cy), :]
        return carry

    def source_copy(k):
        return pltpu.make_async_remote_copy(
            src_ref=src,
            dst_ref=gathered.at[:, pl.ds(k * rows, rows)],
            send_sem=src_send.at[k],
            recv_sem=src_recv.at[k],
            device_id=(gx, lax.rem(gy + k, groups)),
            device_id_type=MESH,
        )

    comps = src.shape[0] // (steps + 1)

    def source_terms():
        contract_last = (((1,), (1,)), ((), ()))
        amplitude = lax.dot_general(
            res_ref[...], hist[...], contract_last, preferred_element_type=jnp.float32
        )
        mech = mech_ref[...].astype(jnp.float32)
        spare = jnp.zeros((comps - mech.shape[0], rows), jnp.float32)
        parts = []
        for t in range(steps):
            parts += [mech * amplitude[t : t + 1, :], spare]
        offsets = off_ref[...]
        places = [own_ref[...], offsets // (cy * cz), (offsets // cz) % cy, offsets % cz]
        places = [p.astype(jnp.float32) for p in places]
        parts += [jnp.concatenate(places + [jnp.zeros((comps - 4, rows), jnp.float32)], axis=0)]
        packed = jnp.concatenate(parts, axis=0).astype(jnp.bfloat16)
        src[...] = packed
        gathered[:, pl.ds(0, rows)] = packed

    def source_masks():
        for k in range(groups):
            lanes = pl.ds(k * rows, rows)
            info = gathered[pl.ds(steps * comps, comps), lanes].astype(jnp.float32)
            cell_plane = info[0:1] * float(cx * cy) + info[1:2] * float(cy) + info[2:3]
            plane = lax.broadcasted_iota(jnp.int32, (cx * cy, rows), 0) + gy * (cx * cy)
            plane_hot[:, lanes] = jnp.where(
                plane == cell_plane.astype(jnp.int32), 1.0, 0.0
            ).astype(jnp.bfloat16)
            height = lax.broadcasted_iota(jnp.int32, (cz, rows), 0)
            level_hot[:, lanes] = jnp.where(
                height == info[3:4].astype(jnp.int32), 1.0, 0.0
            ).astype(jnp.bfloat16)

    def insert_sources(t):
        values = gathered[pl.ds(t * comps, comps), :].astype(jnp.float32)
        for comp in range(0, 6, 2):
            spread = jnp.concatenate(
                [
                    level_hot[...] * values[c : c + 1, :].astype(jnp.bfloat16)
                    for c in (comp, comp + 1)
                ],
                axis=0,
            )
            placed = lax.dot_general(
                plane_hot[...], spread, (((1,), (1,)), ((), ())),
                preferred_element_type=jnp.float32,
            )
            for c in range(2):
                place = S.at[comp + c, pl.ds(XP, cx), pl.ds(YP, cy), :]
                place[...] = place[...] + placed[:, c * cz : (c + 1) * cz].reshape(cx, cy, cz)

    arrivals = (
        (gx > 0).astype(jnp.int32) + (gx < blocks - 1).astype(jnp.int32) + (groups - 1)
    )
    loads[0].wait()
    pl.semaphore_wait(barrier, arrivals)

    def send_stress(phase):
        return lambda side: send_face(side, phase, S, STRESS_FACES)

    def send_velocity(phase):
        return lambda side: send_face(side, phase, V, VELOCITY_FACES)

    for which in (far, near, across):
        at_sides(which, send_stress(0))
    for load in (loads[1],) + tuple(loads[6:]):
        load.wait()
    source_terms()
    for k in range(1, groups):
        source_copy(k).start()
    loads[2].wait()
    loads[3].wait()
    for t in range(steps):
        first, second = 2 * t, 2 * t + 1
        last = t == steps - 1
        lax.fori_loop(0, cx, velocity_inner, 0)
        if t > 0:
            insert_sources(t)
        exchange(first, STRESS_FACES, apply_force, (send_velocity(second),))
        if t == 0:
            loads[4].wait()
            loads[5].wait()
        if t == 0 and last:
            for k in range(1, groups):
                source_copy(k).wait_recv()
            source_masks()
            insert_sources(0)
        lax.fori_loop(0, cx, functools.partial(stress_inner, last), 0)
        if t == 0 and not last:
            for k in range(1, groups):
                source_copy(k).wait_recv()
            source_masks()
            insert_sources(0)
        exchange(
            second, VELOCITY_FACES,
            functools.partial(apply_strain, s_out if last else S),
            () if last else (send_stress(second + 1),),
        )
    for t in range(steps):
        finish_faces(2 * t, STRESS_FACES)
        finish_faces(2 * t + 1, VELOCITY_FACES)
    for k in range(1, groups):
        source_copy(k).wait_send()


def local(
    velocity, stresses, buoyancy, lame_first, rigidity,
    histories, mechanism, resample, owners, cell_offsets,
):
    groups = lax.axis_size("gy")
    blocks = lax.axis_size("gx")
    rows, samples = histories.shape
    steps = resample.shape[1]
    _, cx, cy, cz = velocity.shape
    comps = 8
    tall = comps * (steps + 1)
    f32, bf16 = jnp.float32, jnp.bfloat16
    hbm = pl.BlockSpec(memory_space=pl.ANY)
    vmem = pl.BlockSpec(memory_space=pltpu.VMEM)
    dma = pltpu.SemaphoreType.DMA
    phases = 2 * steps
    return pl.pallas_call(
        functools.partial(kernel, groups, blocks, steps),
        out_shape=(
            pltpu.VMEM(velocity.shape, f32),
            pltpu.VMEM(stresses.shape, f32),
        ),
        in_specs=[hbm] * 10,
        out_specs=(vmem, vmem),
        scratch_shapes=[
            pltpu.VMEM((3, cx + 2 * XP, cy + 2 * YP, cz), f32),
            pltpu.VMEM((6, cx + 2 * XP, cy + 2 * YP, cz), f32),
            pltpu.VMEM((cx, cy, cz), f32),
            pltpu.VMEM((cx, cy, cz), f32),
            pltpu.VMEM((cx, cy, cz), f32),
            pltpu.VMEM((rows, samples), bf16),
            pltpu.VMEM((mechanism.shape[1], rows), bf16),
            pltpu.VMEM((steps, samples), bf16),
            pltpu.VMEM((1, rows), jnp.int32),
            pltpu.VMEM((1, rows), jnp.int32),
            pltpu.VMEM((tall, rows), bf16),
            pltpu.VMEM((tall, groups * rows), bf16),
            pltpu.VMEM((cx * cy, groups * rows), bf16),
            pltpu.VMEM((cz, groups * rows), bf16),
            pltpu.VMEM((phases, 2, 5, cy, cz), f32),
            pltpu.VMEM((phases, 2, 5, cy, cz), f32),
            pltpu.VMEM((phases, 2, 5, cx, cz), f32),
            pltpu.VMEM((phases, 2, 5, cx, cz), f32),
            dma((10,)),
            dma((groups,)),
            dma((groups,)),
            dma((phases, 4)),
            dma((phases, 4)),
        ],
        compiler_params=pltpu.CompilerParams(collective_id=0, has_side_effects=True),
    )(
        velocity, stresses, buoyancy, lame_first, rigidity, histories, mechanism.T, resample.T,
        owners.reshape(1, rows), cell_offsets.reshape(1, rows),
    )


def solution(mesh):
    in_specs = (
        P(None, "gx", "gy", None),
        P(None, "gx", "gy", None),
        P("gx", "gy", None),
        P("gx", "gy", None),
        P("gx", "gy", None),
        P(("gx", "gy"), None),
        P(("gx", "gy"), None),
        P(),
        P(("gx", "gy"), None),
        P(("gx", "gy")),
    )
    out_specs = (P(None, "gx", "gy", None), P(None, "gx", "gy", None))
    return jax.shard_map(local, mesh=mesh, in_specs=in_specs, out_specs=out_specs, check_vma=False)
```

```python
import functools

import jax
import jax.numpy as jnp
from jax import lax
from jax.experimental import pallas as pl
from jax.experimental.pallas import tpu as pltpu
from jax.sharding import PartitionSpec as P

A = 9.0 / 8.0
B = -1.0 / 24.0
MESH = pl.DeviceIdType.MESH
XP = 2
YP = 8

STRESS_FACES = (((0, True), (3, False), (4, False)), ((3, False), (1, True), (5, False)))
VELOCITY_FACES = (((0, False), (1, True), (2, True)), ((0, True), (1, False), (2, True)))


def face_layers(faces, up, extent):
    out = []
    for comp, forward in faces:
        if up:
            out += [(comp, extent - 1, not forward)]
            out += [] if forward else [(comp, extent - 2, False)]
        else:
            out += [(comp, 0, forward)]
            out += [(comp, 1, False)] if forward else []
    return out


def face_slots(faces, up, extent):
    return sum(2 if wide else 1 for _, _, wide in face_layers(faces, up, extent))


def halo_terms(faces, from_low, extent, halo):
    out, at = [], 0
    for comp, forward in faces:
        if from_low == forward:
            sign = -B if from_low else B
            out.append((comp, 0 if from_low else extent - 1, sign * halo(at)))
            at += 1
            continue
        first, second = halo(at) + halo(at + 1), halo(at + 2)
        at += 3
        if from_low:
            out.append((comp, 0, -A * first - B * second))
            out.append((comp, 1, -B * first))
        else:
            out.append((comp, extent - 1, A * first + B * second))
            out.append((comp, extent - 2, B * first))
    return out


def kernel(
    groups, blocks, steps,
    v_hbm, s_hbm, buoy_hbm, lame_hbm, rig_hbm, hist_hbm, mech_hbm, res_hbm, own_hbm, off_hbm,
    v_out, s_out,
    V, S, buoy, lame, rig, hist, mech_ref, res_ref, own_ref, off_ref, src, gathered, plane_hot, level_hot,
    send_x, recv_x, send_y, recv_y,
    stress_sem, load_sem, src_send, src_recv, face_send, face_recv,
):
    gx = lax.axis_index("gx")
    gy = lax.axis_index("gy")
    cx, cy, cz = buoy.shape
    rows = hist.shape[0]
    inner = (slice(None), pl.ds(XP, cx), pl.ds(YP, cy), slice(None))

    barrier = pltpu.get_barrier_semaphore()
    sides = (
        (gx > 0, (gx - 1, gy)),
        (gx < blocks - 1, (gx + 1, gy)),
        (gy > 0, (gx, gy - 1)),
        (gy < groups - 1, (gx, gy + 1)),
    )
    for there, device in sides[:2]:
        @pl.when(there)
        def _(device=device):
            pl.semaphore_signal(barrier, inc=1, device_id=device, device_id_type=MESH)
    for k in range(1, groups):
        pl.semaphore_signal(
            barrier, inc=1, device_id=(gx, lax.rem(gy + k, groups)), device_id_type=MESH
        )

    loads = [
        pltpu.make_async_copy(hist_hbm, hist, load_sem.at[0]),
        pltpu.make_async_copy(v_hbm, V.at[inner], load_sem.at[1]),
        pltpu.make_async_copy(buoy_hbm, buoy, load_sem.at[2]),
        pltpu.make_async_copy(lame_hbm, lame, load_sem.at[3]),
        pltpu.make_async_copy(rig_hbm, rig, load_sem.at[4]),
        pltpu.make_async_copy(mech_hbm, mech_ref, load_sem.at[5]),
        pltpu.make_async_copy(res_hbm, res_ref, load_sem.at[6]),
        pltpu.make_async_copy(own_hbm, own_ref, load_sem.at[7]),
        pltpu.make_async_copy(off_hbm, off_ref, load_sem.at[8]),
    ]
    stress_loads = {
        comp: pltpu.make_async_copy(
            s_hbm.at[comp], S.at[(comp,) + inner[1:]], stress_sem.at[comp]
        )
        for comp in (3, 1, 5, 0, 4, 2)
    }
    for load in list(stress_loads.values()) + loads:
        load.start()

    for ref in (V, S):
        zero_x = jnp.zeros((ref.shape[0], XP, cy, cz), jnp.float32)
        ref[:, pl.ds(0, XP), pl.ds(YP, cy), :] = zero_x
        ref[:, pl.ds(XP + cx, XP), pl.ds(YP, cy), :] = zero_x

        def clear(x, carry, ref=ref):
            zero_y = jnp.zeros((ref.shape[0], YP, cz), jnp.float32)
            ref[:, XP + x, pl.ds(0, YP), :] = zero_y
            ref[:, XP + x, pl.ds(YP + cy, YP), :] = zero_y
            return carry

        lax.fori_loop(0, cx, clear, 0)

    def face_copy(phase, side, faces):
        axis, up = side // 2, side % 2
        send, recv = ((send_x, recv_x), (send_y, recv_y))[axis]
        count = face_slots(faces[axis], bool(up), (cx, cy)[axis])
        return pltpu.make_async_remote_copy(
            src_ref=send.at[phase, up, pl.ds(0, count)],
            dst_ref=recv.at[phase, up, pl.ds(0, count)],
            send_sem=face_send.at[phase, side],
            recv_sem=face_recv.at[phase, side],
            device_id=sides[side][1],
            device_id_type=MESH,
        )

    def row(ref, comp, axis, layer):
        x, y = (XP, YP) if ref is V or ref is S else (0, 0)
        if axis == 0:
            return ref.at[comp, x + layer, pl.ds(y, cy), :]
        return ref.at[comp, pl.ds(x, cx), y + layer, :]

    def coefficient(ref, axis, layer):
        return ref[layer] if axis == 0 else ref[:, layer, :]

    odd = lax.rem(gy, 2) == 1
    even = jnp.logical_not(odd)
    near = ((2, jnp.logical_and(sides[2][0], odd)), (3, jnp.logical_and(sides[3][0], even)))
    far = ((3, jnp.logical_and(sides[3][0], odd)), (2, jnp.logical_and(sides[2][0], even)))
    across = ((0, sides[0][0]), (1, sides[1][0]))

    def send_face(side, phase, ref, faces):
        axis, up = side // 2, side % 2
        send = (send_x, send_y)[axis]
        at = 0
        for comp, layer, wide in face_layers(faces[axis], bool(up), (cx, cy)[axis]):
            value = row(ref, comp, axis, layer)[...]
            head = value.astype(jnp.bfloat16)
            send[phase, up, at] = head
            if wide:
                rest = value - head.astype(jnp.float32)
                send[phase, up, at + 1] = rest.astype(jnp.bfloat16)
            at += 2 if wide else 1
        face_copy(phase, side, faces).start()

    def receive_face(side, phase, faces, apply):
        axis, up = side // 2, side % 2
        recv = (recv_x, recv_y)[axis]
        face_copy(phase, 2 * axis + 1 - up, faces).wait_recv()
        for comp, layer, value in halo_terms(
            faces[axis], not up, (cx, cy)[axis], lambda at: recv[phase, 1 - up, at].astype(jnp.float32)
        ):
            apply(axis, comp, layer, value)

    def at_sides(which, *actions):
        for side, there in which:
            @pl.when(there)
            def _(side=side):
                for action in actions:
                    action(side)

    def exchange(phase, faces, apply, send):
        def receive(side):
            receive_face(side, phase, faces, apply)

        at_sides(across, receive)
        at_sides(near, receive, *send)
        at_sides(far, receive, *send)
        at_sides(across, *send)

    def finish_faces(phase, faces):
        for side in (0, 1, 2, 3):
            @pl.when(sides[side][0])
            def _(side=side):
                face_copy(phase, side, faces).wait_send()

    def add(ref, comp, axis, layer, value):
        place = row(ref, comp, axis, layer)
        place[...] = place[...] + value

    force_of = ({0: 0, 3: 1, 4: 2}, {3: 0, 1: 1, 5: 2})

    def apply_force(axis, comp, layer, value):
        add(V, force_of[axis][comp], axis, layer, coefficient(buoy, axis, layer) * value)

    shear_of = ({1: 3, 2: 4}, {0: 3, 2: 5})

    def apply_strain(target, axis, comp, layer, value):
        mu = coefficient(rig, axis, layer)
        if comp != axis:
            add(target, shear_of[axis][comp], axis, layer, mu * value)
            return
        volume = coefficient(lame, axis, layer) * value
        for normal in range(3):
            extra = volume + 2.0 * mu * value if normal == axis else volume
            add(target, normal, axis, layer, extra)

    level = lax.broadcasted_iota(jnp.int32, (cy, cz), 1)

    def along_z(values, by):
        moved = pltpu.roll(values, (-by) % cz, 1)
        return jnp.where(level < cz - by if by > 0 else level >= -by, moved, 0.0)

    def differ(ref, comp, x, dimension, forward):
        def window(by):
            if dimension == 0:
                return ref[comp, XP + x + by, pl.ds(YP, cy), :]
            if dimension == 1:
                return ref[comp, XP + x, pl.ds(YP + by, cy), :]
            values = ref[comp, XP + x, pl.ds(YP, cy), :]
            return along_z(values, by) if by else values

        if forward:
            return A * (window(1) - window(0)) + B * (window(2) - window(-1))
        return A * (window(0) - window(-1)) + B * (window(1) - window(-2))

    def velocity_inner(x, carry):
        force = (
            differ(S, 0, x, 0, True) + differ(S, 3, x, 1, False) + differ(S, 4, x, 2, False),
            differ(S, 3, x, 0, False) + differ(S, 1, x, 1, True) + differ(S, 5, x, 2, False),
            differ(S, 4, x, 0, False) + differ(S, 5, x, 1, False) + differ(S, 2, x, 2, True),
        )
        factor = buoy[x]
        for comp in range(3):
            place = V.at[comp, XP + x, pl.ds(YP, cy), :]
            place[...] = place[...] + factor * force[comp]
        return carry

    def stress_inner(last, x, carry):
        one = differ(V, 0, x, 0, False)
        two = differ(V, 1, x, 1, False)
        three = differ(V, 2, x, 2, False)
        mu = rig[x]
        volume = lame[x] * (one + two + three)
        rates = (
            volume + 2.0 * mu * one,
            volume + 2.0 * mu * two,
            volume + 2.0 * mu * three,
            mu * (differ(V, 0, x, 1, True) + differ(V, 1, x, 0, True)),
            mu * (differ(V, 0, x, 2, True) + differ(V, 2, x, 0, True)),
            mu * (differ(V, 1, x, 2, True) + differ(V, 2, x, 1, True)),
        )
        for comp in range(6):
            place = S.at[comp, XP + x, pl.ds(YP, cy), :]
            target = s_out.at[comp, x] if last else place
            target[...] = place[...] + rates[comp]
        if last:
            for comp in range(3):
                v_out[comp, x] = V[comp, XP + x, pl.ds(YP, cy), :]
        return carry

    def source_copy(k):
        return pltpu.make_async_remote_copy(
            src_ref=src,
            dst_ref=gathered.at[:, pl.ds(k * rows, rows)],
            send_sem=src_send.at[k],
            recv_sem=src_recv.at[k],
            device_id=(gx, lax.rem(gy + k, groups)),
            device_id_type=MESH,
        )

    comps = src.shape[0] // (steps + 1)

    def source_terms():
        contract_last = (((1,), (1,)), ((), ()))
        amplitude = lax.dot_general(
            res_ref[...], hist[...], contract_last, preferred_element_type=jnp.float32
        )
        mech = mech_ref[...].astype(jnp.float32)
        spare = jnp.zeros((comps - mech.shape[0], rows), jnp.float32)
        parts = []
        for t in range(steps):
            parts += [mech * amplitude[t : t + 1, :], spare]
        offsets = off_ref[...]
        places = [own_ref[...], offsets // (cy * cz), (offsets // cz) % cy, offsets % cz]
        places = [p.astype(jnp.float32) for p in places]
        parts += [jnp.concatenate(places + [jnp.zeros((comps - 4, rows), jnp.float32)], axis=0)]
        packed = jnp.concatenate(parts, axis=0).astype(jnp.bfloat16)
        src[...] = packed
        gathered[:, pl.ds(0, rows)] = packed

    def source_masks():
        for k in range(groups):
            lanes = pl.ds(k * rows, rows)
            info = gathered[pl.ds(steps * comps, comps), lanes].astype(jnp.float32)
            cell_plane = info[0:1] * float(cx * cy) + info[1:2] * float(cy) + info[2:3]
            plane = lax.broadcasted_iota(jnp.int32, (cx * cy, rows), 0) + gy * (cx * cy)
            plane_hot[:, lanes] = jnp.where(
                plane == cell_plane.astype(jnp.int32), 1.0, 0.0
            ).astype(jnp.bfloat16)
            height = lax.broadcasted_iota(jnp.int32, (cz, rows), 0)
            level_hot[:, lanes] = jnp.where(
                height == info[3:4].astype(jnp.int32), 1.0, 0.0
            ).astype(jnp.bfloat16)

    def insert_sources(t):
        values = gathered[pl.ds(t * comps, comps), :].astype(jnp.float32)
        for comp in range(0, 6, 2):
            spread = jnp.concatenate(
                [
                    level_hot[...] * values[c : c + 1, :].astype(jnp.bfloat16)
                    for c in (comp, comp + 1)
                ],
                axis=0,
            )
            placed = lax.dot_general(
                plane_hot[...], spread, (((1,), (1,)), ((), ())),
                preferred_element_type=jnp.float32,
            )
            for c in range(2):
                place = S.at[comp + c, pl.ds(XP, cx), pl.ds(YP, cy), :]
                place[...] = place[...] + placed[:, c * cz : (c + 1) * cz].reshape(cx, cy, cz)

    arrivals = (
        (gx > 0).astype(jnp.int32) + (gx < blocks - 1).astype(jnp.int32) + (groups - 1)
    )
    pl.semaphore_wait(barrier, arrivals)

    def send_stress(phase):
        return lambda side: send_face(side, phase, S, STRESS_FACES)

    def send_velocity(phase):
        return lambda side: send_face(side, phase, V, VELOCITY_FACES)

    for comp, _ in STRESS_FACES[1]:
        stress_loads.pop(comp).wait()
    at_sides(far, send_stress(0))
    at_sides(near, send_stress(0))
    for load in stress_loads.values():
        load.wait()
    at_sides(across, send_stress(0))
    for load in [loads[0]] + loads[5:]:
        load.wait()
    source_terms()
    for k in range(1, groups):
        source_copy(k).start()
    loads[1].wait()
    loads[2].wait()
    for t in range(steps):
        first, second = 2 * t, 2 * t + 1
        last = t == steps - 1
        lax.fori_loop(0, cx, velocity_inner, 0)
        if t > 0:
            insert_sources(t)
        exchange(first, STRESS_FACES, apply_force, (send_velocity(second),))
        if t == 0:
            loads[3].wait()
            loads[4].wait()
        if t == 0 and last:
            for k in range(1, groups):
                source_copy(k).wait_recv()
            source_masks()
            insert_sources(0)
        lax.fori_loop(0, cx, functools.partial(stress_inner, last), 0)
        if t == 0 and not last:
            for k in range(1, groups):
                source_copy(k).wait_recv()
            source_masks()
            insert_sources(0)
        exchange(
            second, VELOCITY_FACES,
            functools.partial(apply_strain, s_out if last else S),
            () if last else (send_stress(second + 1),),
        )
    for t in range(steps):
        finish_faces(2 * t, STRESS_FACES)
        finish_faces(2 * t + 1, VELOCITY_FACES)
    for k in range(1, groups):
        source_copy(k).wait_send()


def store_kernel(v_ref, s_ref, v_out, s_out, sem):
    copies = [pltpu.make_async_copy(v_ref, v_out, sem.at[0])]
    half = s_ref.shape[0] // 2
    for part in range(2):
        layers = pl.ds(part * half, half)
        copies.append(pltpu.make_async_copy(s_ref.at[layers], s_out.at[layers], sem.at[1 + part]))
    for copy in copies:
        copy.start()
    for copy in copies:
        copy.wait()


def local(
    velocity, stresses, buoyancy, lame_first, rigidity,
    histories, mechanism, resample, owners, cell_offsets,
):
    groups = lax.axis_size("gy")
    blocks = lax.axis_size("gx")
    rows, samples = histories.shape
    steps = resample.shape[1]
    _, cx, cy, cz = velocity.shape
    comps = 8
    tall = comps * (steps + 1)
    f32, bf16 = jnp.float32, jnp.bfloat16
    hbm = pl.BlockSpec(memory_space=pl.ANY)
    vmem = pl.BlockSpec(memory_space=pltpu.VMEM)
    dma = pltpu.SemaphoreType.DMA
    phases = 2 * steps
    v_last, s_last = pl.pallas_call(
        functools.partial(kernel, groups, blocks, steps),
        out_shape=(
            pltpu.VMEM(velocity.shape, f32),
            pltpu.VMEM(stresses.shape, f32),
        ),
        in_specs=[hbm] * 10,
        out_specs=(vmem, vmem),
        scratch_shapes=[
            pltpu.VMEM((3, cx + 2 * XP, cy + 2 * YP, cz), f32),
            pltpu.VMEM((6, cx + 2 * XP, cy + 2 * YP, cz), f32),
            pltpu.VMEM((cx, cy, cz), f32),
            pltpu.VMEM((cx, cy, cz), f32),
            pltpu.VMEM((cx, cy, cz), f32),
            pltpu.VMEM((rows, samples), bf16),
            pltpu.VMEM((mechanism.shape[1], rows), bf16),
            pltpu.VMEM((steps, samples), bf16),
            pltpu.VMEM((1, rows), jnp.int32),
            pltpu.VMEM((1, rows), jnp.int32),
            pltpu.VMEM((tall, rows), bf16),
            pltpu.VMEM((tall, groups * rows), bf16),
            pltpu.VMEM((cx * cy, groups * rows), bf16),
            pltpu.VMEM((cz, groups * rows), bf16),
            pltpu.VMEM((phases, 2, 9, cy, cz), bf16),
            pltpu.VMEM((phases, 2, 9, cy, cz), bf16),
            pltpu.VMEM((phases, 2, 9, cx, cz), bf16),
            pltpu.VMEM((phases, 2, 9, cx, cz), bf16),
            dma((6,)),
            dma((9,)),
            dma((groups,)),
            dma((groups,)),
            dma((phases, 4)),
            dma((phases, 4)),
        ],
        compiler_params=pltpu.CompilerParams(collective_id=0, has_side_effects=True),
    )(
        velocity, stresses, buoyancy, lame_first, rigidity, histories, mechanism.T, resample.T,
        owners.reshape(1, rows), cell_offsets.reshape(1, rows),
    )
    return pl.pallas_call(
        store_kernel,
        out_shape=(
            jax.ShapeDtypeStruct(velocity.shape, f32),
            jax.ShapeDtypeStruct(stresses.shape, f32),
        ),
        in_specs=[vmem, vmem],
        out_specs=(hbm, hbm),
        scratch_shapes=[dma((3,))],
    )(
        pltpu.with_memory_space_constraint(v_last, pltpu.VMEM),
        pltpu.with_memory_space_constraint(s_last, pltpu.VMEM),
    )


def solution(mesh):
    in_specs = (
        P(None, "gx", "gy", None),
        P(None, "gx", "gy", None),
        P("gx", "gy", None),
        P("gx", "gy", None),
        P("gx", "gy", None),
        P(("gx", "gy"), None),
        P(("gx", "gy"), None),
        P(),
        P(("gx", "gy"), None),
        P(("gx", "gy")),
    )
    out_specs = (P(None, "gx", "gy", None), P(None, "gx", "gy", None))
    return jax.shard_map(local, mesh=mesh, in_specs=in_specs, out_specs=out_specs, check_vma=False)
```

```python
import functools

import jax
import jax.numpy as jnp
from jax import lax
from jax.experimental import pallas as pl
from jax.experimental.pallas import tpu as pltpu
from jax.sharding import PartitionSpec as P

A = 9.0 / 8.0
B = -1.0 / 24.0
MESH = pl.DeviceIdType.MESH
XP = 2
YP = 8

STRESS_FACES = (((0, True), (3, False), (4, False)), ((3, False), (1, True), (5, False)))
VELOCITY_FACES = (((0, False), (1, True), (2, True)), ((0, True), (1, False), (2, True)))


def face_layers(faces, up, extent):
    out = []
    for comp, forward in faces:
        if up:
            out += [(comp, extent - 1, not forward)]
            out += [] if forward else [(comp, extent - 2, False)]
        else:
            out += [(comp, 0, forward)]
            out += [(comp, 1, False)] if forward else []
    return out


def face_slots(faces, up, extent):
    return sum(2 if wide else 1 for _, _, wide in face_layers(faces, up, extent))


def halo_terms(faces, from_low, extent, halo):
    out, at = [], 0
    for comp, forward in faces:
        if from_low == forward:
            sign = -B if from_low else B
            out.append((comp, 0 if from_low else extent - 1, sign * halo(at)))
            at += 1
            continue
        first, second = halo(at) + halo(at + 1), halo(at + 2)
        at += 3
        if from_low:
            out.append((comp, 0, -A * first - B * second))
            out.append((comp, 1, -B * first))
        else:
            out.append((comp, extent - 1, A * first + B * second))
            out.append((comp, extent - 2, B * first))
    return out


def kernel(
    groups, blocks, steps,
    v_hbm, s_hbm, buoy_hbm, lame_hbm, rig_hbm, hist_hbm, mech_hbm, res_hbm, own_hbm, off_hbm,
    v_out, s_out,
    V, S, buoy, lame, rig, hist, mech_ref, res_ref, own_ref, off_ref, src, gathered, plane_hot, level_hot,
    send_x, recv_x, send_y, recv_y,
    stress_sem, load_sem, src_send, src_recv, face_send, face_recv,
):
    gx = lax.axis_index("gx")
    gy = lax.axis_index("gy")
    cx, cy, cz = buoy.shape
    rows = hist.shape[0]
    inner = (slice(None), pl.ds(XP, cx), pl.ds(YP, cy), slice(None))

    barrier = pltpu.get_barrier_semaphore()
    sides = (
        (gx > 0, (gx - 1, gy)),
        (gx < blocks - 1, (gx + 1, gy)),
        (gy > 0, (gx, gy - 1)),
        (gy < groups - 1, (gx, gy + 1)),
    )
    for there, device in sides[:2]:
        @pl.when(there)
        def _(device=device):
            pl.semaphore_signal(barrier, inc=1, device_id=device, device_id_type=MESH)
    for k in range(1, groups):
        pl.semaphore_signal(
            barrier, inc=1, device_id=(gx, lax.rem(gy + k, groups)), device_id_type=MESH
        )

    loads = [
        pltpu.make_async_copy(hist_hbm, hist, load_sem.at[0]),
        pltpu.make_async_copy(v_hbm, V.at[inner], load_sem.at[1]),
        pltpu.make_async_copy(buoy_hbm, buoy, load_sem.at[2]),
        pltpu.make_async_copy(lame_hbm, lame, load_sem.at[3]),
        pltpu.make_async_copy(rig_hbm, rig, load_sem.at[4]),
        pltpu.make_async_copy(mech_hbm, mech_ref, load_sem.at[5]),
        pltpu.make_async_copy(res_hbm, res_ref, load_sem.at[6]),
        pltpu.make_async_copy(own_hbm, own_ref, load_sem.at[7]),
        pltpu.make_async_copy(off_hbm, off_ref, load_sem.at[8]),
    ]
    stress_loads = {
        comp: pltpu.make_async_copy(
            s_hbm.at[comp], S.at[(comp,) + inner[1:]], stress_sem.at[comp]
        )
        for comp in (3, 1, 5, 0, 4, 2)
    }
    for load in list(stress_loads.values()) + loads:
        load.start()

    for ref in (V, S):
        zero_x = jnp.zeros((ref.shape[0], XP, cy, cz), jnp.float32)
        ref[:, pl.ds(0, XP), pl.ds(YP, cy), :] = zero_x
        ref[:, pl.ds(XP + cx, XP), pl.ds(YP, cy), :] = zero_x

        def clear(x, carry, ref=ref):
            zero_y = jnp.zeros((ref.shape[0], YP, cz), jnp.float32)
            ref[:, XP + x, pl.ds(0, YP), :] = zero_y
            ref[:, XP + x, pl.ds(YP + cy, YP), :] = zero_y
            return carry

        lax.fori_loop(0, cx, clear, 0)

    def face_copy(phase, side, faces):
        axis, up = side // 2, side % 2
        send, recv = ((send_x, recv_x), (send_y, recv_y))[axis]
        count = face_slots(faces[axis], bool(up), (cx, cy)[axis])
        return pltpu.make_async_remote_copy(
            src_ref=send.at[phase, up, pl.ds(0, count)],
            dst_ref=recv.at[phase, up, pl.ds(0, count)],
            send_sem=face_send.at[phase, side],
            recv_sem=face_recv.at[phase, side],
            device_id=sides[side][1],
            device_id_type=MESH,
        )

    def row(ref, comp, axis, layer):
        x, y = (XP, YP) if ref is V or ref is S else (0, 0)
        if axis == 0:
            return ref.at[comp, x + layer, pl.ds(y, cy), :]
        return ref.at[comp, pl.ds(x, cx), y + layer, :]

    def coefficient(ref, axis, layer):
        return ref[layer] if axis == 0 else ref[:, layer, :]

    odd = lax.rem(gy, 2) == 1
    even = jnp.logical_not(odd)
    near = ((2, jnp.logical_and(sides[2][0], odd)), (3, jnp.logical_and(sides[3][0], even)))
    far = ((3, jnp.logical_and(sides[3][0], odd)), (2, jnp.logical_and(sides[2][0], even)))
    across = ((0, sides[0][0]), (1, sides[1][0]))

    def send_face(side, phase, ref, faces):
        axis, up = side // 2, side % 2
        send = (send_x, send_y)[axis]
        at = 0
        for comp, layer, wide in face_layers(faces[axis], bool(up), (cx, cy)[axis]):
            value = row(ref, comp, axis, layer)[...]
            head = value.astype(jnp.bfloat16)
            send[phase, up, at] = head
            if wide:
                rest = value - head.astype(jnp.float32)
                send[phase, up, at + 1] = rest.astype(jnp.bfloat16)
            at += 2 if wide else 1
        face_copy(phase, side, faces).start()

    def receive_face(side, phase, faces, apply):
        axis, up = side // 2, side % 2
        recv = (recv_x, recv_y)[axis]
        face_copy(phase, 2 * axis + 1 - up, faces).wait_recv()
        for comp, layer, value in halo_terms(
            faces[axis], not up, (cx, cy)[axis], lambda at: recv[phase, 1 - up, at].astype(jnp.float32)
        ):
            apply(axis, comp, layer, value)

    def at_sides(which, *actions):
        for side, there in which:
            @pl.when(there)
            def _(side=side):
                for action in actions:
                    action(side)

    def exchange(phase, faces, apply, send):
        def receive(side):
            receive_face(side, phase, faces, apply)

        at_sides(across, receive)
        at_sides(near, receive, *send)
        at_sides(far, receive, *send)
        at_sides(across, *send)

    def finish_faces(phase, faces):
        for side in (0, 1, 2, 3):
            @pl.when(sides[side][0])
            def _(side=side):
                face_copy(phase, side, faces).wait_send()

    def add(ref, comp, axis, layer, value):
        place = row(ref, comp, axis, layer)
        place[...] = place[...] + value

    force_of = ({0: 0, 3: 1, 4: 2}, {3: 0, 1: 1, 5: 2})

    def apply_force(axis, comp, layer, value):
        add(V, force_of[axis][comp], axis, layer, coefficient(buoy, axis, layer) * value)

    shear_of = ({1: 3, 2: 4}, {0: 3, 2: 5})

    def apply_strain(target, axis, comp, layer, value):
        mu = coefficient(rig, axis, layer)
        if comp != axis:
            add(target, shear_of[axis][comp], axis, layer, mu * value)
            return
        volume = coefficient(lame, axis, layer) * value
        for normal in range(3):
            extra = volume + 2.0 * mu * value if normal == axis else volume
            add(target, normal, axis, layer, extra)

    level = lax.broadcasted_iota(jnp.int32, (cy, cz), 1)

    def along_z(values, by):
        moved = pltpu.roll(values, (-by) % cz, 1)
        return jnp.where(level < cz - by if by > 0 else level >= -by, moved, 0.0)

    def differ(ref, comp, x, dimension, forward):
        def window(by):
            if dimension == 0:
                return ref[comp, XP + x + by, pl.ds(YP, cy), :]
            if dimension == 1:
                return ref[comp, XP + x, pl.ds(YP + by, cy), :]
            values = ref[comp, XP + x, pl.ds(YP, cy), :]
            return along_z(values, by) if by else values

        if forward:
            return A * (window(1) - window(0)) + B * (window(2) - window(-1))
        return A * (window(0) - window(-1)) + B * (window(1) - window(-2))

    def velocity_inner(x, carry):
        force = (
            differ(S, 0, x, 0, True) + differ(S, 3, x, 1, False) + differ(S, 4, x, 2, False),
            differ(S, 3, x, 0, False) + differ(S, 1, x, 1, True) + differ(S, 5, x, 2, False),
            differ(S, 4, x, 0, False) + differ(S, 5, x, 1, False) + differ(S, 2, x, 2, True),
        )
        factor = buoy[x]
        for comp in range(3):
            place = V.at[comp, XP + x, pl.ds(YP, cy), :]
            place[...] = place[...] + factor * force[comp]
        return carry

    def stress_inner(last, x, carry):
        one = differ(V, 0, x, 0, False)
        two = differ(V, 1, x, 1, False)
        three = differ(V, 2, x, 2, False)
        mu = rig[x]
        volume = lame[x] * (one + two + three)
        rates = (
            volume + 2.0 * mu * one,
            volume + 2.0 * mu * two,
            volume + 2.0 * mu * three,
            mu * (differ(V, 0, x, 1, True) + differ(V, 1, x, 0, True)),
            mu * (differ(V, 0, x, 2, True) + differ(V, 2, x, 0, True)),
            mu * (differ(V, 1, x, 2, True) + differ(V, 2, x, 1, True)),
        )
        for comp in range(6):
            place = S.at[comp, XP + x, pl.ds(YP, cy), :]
            target = s_out.at[comp, x] if last else place
            target[...] = place[...] + rates[comp]
        if last:
            for comp in range(3):
                v_out[comp, x] = V[comp, XP + x, pl.ds(YP, cy), :]
        return carry

    def sweep(body):
        batch = 2 if cx % 2 == 0 else 1

        def several(at, carry):
            for one in range(batch):
                carry = body(batch * at + one, carry)
            return carry

        lax.fori_loop(0, cx // batch, several, 0)

    def source_copy(k):
        return pltpu.make_async_remote_copy(
            src_ref=src,
            dst_ref=gathered.at[:, pl.ds(k * rows, rows)],
            send_sem=src_send.at[k],
            recv_sem=src_recv.at[k],
            device_id=(gx, lax.rem(gy + k, groups)),
            device_id_type=MESH,
        )

    comps = src.shape[0] // (steps + 1)

    def source_terms():
        contract_last = (((1,), (1,)), ((), ()))
        amplitude = lax.dot_general(
            res_ref[...], hist[...], contract_last, preferred_element_type=jnp.float32
        )
        mech = mech_ref[...].astype(jnp.float32)
        spare = jnp.zeros((comps - mech.shape[0], rows), jnp.float32)
        parts = []
        for t in range(steps):
            parts += [mech * amplitude[t : t + 1, :], spare]
        offsets = off_ref[...]
        places = [own_ref[...], offsets // (cy * cz), (offsets // cz) % cy, offsets % cz]
        places = [p.astype(jnp.float32) for p in places]
        parts += [jnp.concatenate(places + [jnp.zeros((comps - 4, rows), jnp.float32)], axis=0)]
        packed = jnp.concatenate(parts, axis=0).astype(jnp.bfloat16)
        src[...] = packed
        gathered[:, pl.ds(0, rows)] = packed

    def source_masks():
        for k in range(groups):
            lanes = pl.ds(k * rows, rows)
            info = gathered[pl.ds(steps * comps, comps), lanes].astype(jnp.float32)
            cell_plane = info[0:1] * float(cx * cy) + info[1:2] * float(cy) + info[2:3]
            plane = lax.broadcasted_iota(jnp.int32, (cx * cy, rows), 0) + gy * (cx * cy)
            plane_hot[:, lanes] = jnp.where(
                plane == cell_plane.astype(jnp.int32), 1.0, 0.0
            ).astype(jnp.bfloat16)
            height = lax.broadcasted_iota(jnp.int32, (cz, rows), 0)
            level_hot[:, lanes] = jnp.where(
                height == info[3:4].astype(jnp.int32), 1.0, 0.0
            ).astype(jnp.bfloat16)

    def insert_sources(t):
        values = gathered[pl.ds(t * comps, comps), :].astype(jnp.float32)
        for comp in range(0, 6, 2):
            spread = jnp.concatenate(
                [
                    level_hot[...] * values[c : c + 1, :].astype(jnp.bfloat16)
                    for c in (comp, comp + 1)
                ],
                axis=0,
            )
            placed = lax.dot_general(
                plane_hot[...], spread, (((1,), (1,)), ((), ())),
                preferred_element_type=jnp.float32,
            )
            for c in range(2):
                place = S.at[comp + c, pl.ds(XP, cx), pl.ds(YP, cy), :]
                place[...] = place[...] + placed[:, c * cz : (c + 1) * cz].reshape(cx, cy, cz)

    arrivals = (
        (gx > 0).astype(jnp.int32) + (gx < blocks - 1).astype(jnp.int32) + (groups - 1)
    )
    pl.semaphore_wait(barrier, arrivals)

    def send_stress(phase):
        return lambda side: send_face(side, phase, S, STRESS_FACES)

    def send_velocity(phase):
        return lambda side: send_face(side, phase, V, VELOCITY_FACES)

    for comp, _ in STRESS_FACES[1]:
        stress_loads.pop(comp).wait()
    at_sides(far, send_stress(0))
    at_sides(near, send_stress(0))
    for load in stress_loads.values():
        load.wait()
    at_sides(across, send_stress(0))
    for load in [loads[0]] + loads[5:]:
        load.wait()
    source_terms()
    for k in range(1, groups):
        source_copy(k).start()
    loads[1].wait()
    loads[2].wait()
    for t in range(steps):
        first, second = 2 * t, 2 * t + 1
        last = t == steps - 1
        sweep(velocity_inner)
        if t > 0:
            insert_sources(t)
        exchange(first, STRESS_FACES, apply_force, (send_velocity(second),))
        if t == 0:
            loads[3].wait()
            loads[4].wait()
        if t == 0 and last:
            for k in range(1, groups):
                source_copy(k).wait_recv()
            source_masks()
            insert_sources(0)
        sweep(functools.partial(stress_inner, last))
        if t == 0 and not last:
            for k in range(1, groups):
                source_copy(k).wait_recv()
            source_masks()
            insert_sources(0)
        exchange(
            second, VELOCITY_FACES,
            functools.partial(apply_strain, s_out if last else S),
            () if last else (send_stress(second + 1),),
        )
    for t in range(steps):
        finish_faces(2 * t, STRESS_FACES)
        finish_faces(2 * t + 1, VELOCITY_FACES)
    for k in range(1, groups):
        source_copy(k).wait_send()


def store_kernel(v_ref, s_ref, v_out, s_out, sem):
    copies = [pltpu.make_async_copy(v_ref, v_out, sem.at[0])]
    half = s_ref.shape[0] // 2
    for part in range(2):
        layers = pl.ds(part * half, half)
        copies.append(pltpu.make_async_copy(s_ref.at[layers], s_out.at[layers], sem.at[1 + part]))
    for copy in copies:
        copy.start()
    for copy in copies:
        copy.wait()


def local(
    velocity, stresses, buoyancy, lame_first, rigidity,
    histories, mechanism, resample, owners, cell_offsets,
):
    groups = lax.axis_size("gy")
    blocks = lax.axis_size("gx")
    rows, samples = histories.shape
    steps = resample.shape[1]
    _, cx, cy, cz = velocity.shape
    comps = 8
    tall = comps * (steps + 1)
    f32, bf16 = jnp.float32, jnp.bfloat16
    hbm = pl.BlockSpec(memory_space=pl.ANY)
    vmem = pl.BlockSpec(memory_space=pltpu.VMEM)
    dma = pltpu.SemaphoreType.DMA
    phases = 2 * steps
    v_last, s_last = pl.pallas_call(
        functools.partial(kernel, groups, blocks, steps),
        out_shape=(
            pltpu.VMEM(velocity.shape, f32),
            pltpu.VMEM(stresses.shape, f32),
        ),
        in_specs=[hbm] * 10,
        out_specs=(vmem, vmem),
        scratch_shapes=[
            pltpu.VMEM((3, cx + 2 * XP, cy + 2 * YP, cz), f32),
            pltpu.VMEM((6, cx + 2 * XP, cy + 2 * YP, cz), f32),
            pltpu.VMEM((cx, cy, cz), f32),
            pltpu.VMEM((cx, cy, cz), f32),
            pltpu.VMEM((cx, cy, cz), f32),
            pltpu.VMEM((rows, samples), bf16),
            pltpu.VMEM((mechanism.shape[1], rows), bf16),
            pltpu.VMEM((steps, samples), bf16),
            pltpu.VMEM((1, rows), jnp.int32),
            pltpu.VMEM((1, rows), jnp.int32),
            pltpu.VMEM((tall, rows), bf16),
            pltpu.VMEM((tall, groups * rows), bf16),
            pltpu.VMEM((cx * cy, groups * rows), bf16),
            pltpu.VMEM((cz, groups * rows), bf16),
            pltpu.VMEM((phases, 2, 9, cy, cz), bf16),
            pltpu.VMEM((phases, 2, 9, cy, cz), bf16),
            pltpu.VMEM((phases, 2, 9, cx, cz), bf16),
            pltpu.VMEM((phases, 2, 9, cx, cz), bf16),
            dma((6,)),
            dma((9,)),
            dma((groups,)),
            dma((groups,)),
            dma((phases, 4)),
            dma((phases, 4)),
        ],
        compiler_params=pltpu.CompilerParams(collective_id=0, has_side_effects=True),
    )(
        velocity, stresses, buoyancy, lame_first, rigidity, histories, mechanism.T, resample.T,
        owners.reshape(1, rows), cell_offsets.reshape(1, rows),
    )
    return pl.pallas_call(
        store_kernel,
        out_shape=(
            jax.ShapeDtypeStruct(velocity.shape, f32),
            jax.ShapeDtypeStruct(stresses.shape, f32),
        ),
        in_specs=[vmem, vmem],
        out_specs=(hbm, hbm),
        scratch_shapes=[dma((3,))],
    )(
        pltpu.with_memory_space_constraint(v_last, pltpu.VMEM),
        pltpu.with_memory_space_constraint(s_last, pltpu.VMEM),
    )


def solution(mesh):
    in_specs = (
        P(None, "gx", "gy", None),
        P(None, "gx", "gy", None),
        P("gx", "gy", None),
        P("gx", "gy", None),
        P("gx", "gy", None),
        P(("gx", "gy"), None),
        P(("gx", "gy"), None),
        P(),
        P(("gx", "gy"), None),
        P(("gx", "gy")),
    )
    out_specs = (P(None, "gx", "gy", None), P(None, "gx", "gy", None))
    return jax.shard_map(local, mesh=mesh, in_specs=in_specs, out_specs=out_specs, check_vma=False)
```
